256 devices in a mesh: dp: 64 (over z, x, core), seq: 4 (over y).
Axes of the slice: x: 4, y: 4, z: 8, core: 2. Of those that a mesh axis runs over, the one named last changes fastest.
Arguments:
- tokens: bfloat16 [36864, 3584], P('dp'), may hold values from -6 to 6
- positions: int32 [3, 36864], P(None, 'dp'), may hold values from 0 to 2047
- loss_mask: int32 [36864], P('dp'), may hold values from 0 to 1, as said below
- sample_tokens: int32 [64, 3], replicated, may hold values from 96 to 384, as said below
- dest_slot: int32 [36864], P('dp'), may hold values from 0 to 49151, as said below
- norm_gain: float32 [3584], replicated, may hold values from 0.5 to 1.5
- q_weight: bfloat16 [3584, 2048], P(None, 'seq'), may hold values from -0.09375 to 0.09375
- k_weight: bfloat16 [3584, 512], P(None, 'seq'), may hold values from -0.09375 to 0.09375
- v_weight: bfloat16 [3584, 512], P(None, 'seq'), may hold values from -0.09375 to 0.09375
- q_bias: float32 [2048], P('seq'), may hold values from -3 to 3
- k_bias: float32 [512], P('seq'), may hold values from -3 to 3
- v_bias: float32 [512], P('seq'), may hold values from -3 to 3
- o_weight: bfloat16 [2048, 3584], P('seq'), may hold values from -0.125 to 0.125
Outputs:
- mixed: bfloat16 [49152, 3584], P(('dp', 'seq'))
- token_weight: float32 [49152], P(('dp', 'seq'))
The draws below stay inside these ranges and needn't reach their ends.
Inputs may be any that keep to these rules, and one draw needn't show every extreme that they name: `sample_tokens`: row r gives the token counts of the samples in the buckets of receiver r, of 384, 192 and 192 slots; each count lies between half of its bucket's slots and all of them. Some receiver has all three buckets full. All counts together equal the number of rows of tokens. `dest_slot`: every row has a slot of its own, and the slots that rows take are exactly the first sample_tokens[r, b] slots of each bucket b of each receiver r. Of the rows of one sender at most 12 go to one receiver; a receiver whose buckets are all full takes exactly 12 rows from every sender. `loss_mask`: the first of each sender's 576 rows is 1.
All inputs are finite; a program needn't handle non-finite values.
Results may differ from the reference program's by a relative error of at most 0.015.
Values may be sent and summed in bfloat16 or wider, within the bound.
A program may use at most 128 MiB of HBM per device.

```python
import math
import jax
import jax.numpy as jnp
from jax import lax

D = 3584
HQ = 16
KV = 4
DH = 128
BUCKET = 384
SRC = 576
N_DP = 64
N_SEQ = 4


def plan_tables(key):
    pairing_key = jax.random.fold_in(key, 11)
    length_key = jax.random.fold_in(key, 12)
    shuffle_key = jax.random.fold_in(key, 13)
    half_bucket = BUCKET // 2
    bucket_sizes = jnp.array([BUCKET, half_bucket, half_bucket], jnp.int32)
    pairing = jax.random.permutation(pairing_key, N_DP).astype(jnp.int32)
    pair_count = N_DP // 2
    first_lengths = jax.random.randint(length_key, (pair_count, 3), bucket_sizes // 2, bucket_sizes + 1).astype(jnp.int32)
    first_lengths = first_lengths.at[0].set(bucket_sizes)
    second_lengths = (3 * bucket_sizes // 2 - first_lengths).astype(jnp.int32)
    lengths = jnp.zeros((N_DP, 3), jnp.int32).at[pairing[0::2]].set(first_lengths).at[pairing[1::2]].set(second_lengths)
    local_slot = jnp.arange(2 * BUCKET, dtype=jnp.int32)
    bucket_id = (local_slot >= BUCKET).astype(jnp.int32) + (local_slot >= BUCKET + half_bucket).astype(jnp.int32)
    starts = jnp.array([0, BUCKET, BUCKET + half_bucket], jnp.int32)
    offset = local_slot - starts[bucket_id]
    filled = (offset[None, :] < lengths[:, bucket_id]).reshape(-1).astype(jnp.int32)
    order_index = (jnp.cumsum(filled) - 1).astype(jnp.int32)
    sender = order_index % N_DP
    within = jnp.clip(order_index // N_DP, 0, SRC - 1)
    sender_keys = jax.random.split(shuffle_key, N_DP)
    shuffles = jax.vmap(lambda one_key: jax.random.permutation(one_key, SRC))(sender_keys).astype(jnp.int32)
    source_row = (sender * SRC + shuffles[sender, within]).astype(jnp.int32)
    target = jnp.where(filled > 0, source_row, N_DP * SRC)
    global_slot = jnp.arange(N_DP * 2 * BUCKET, dtype=jnp.int32)
    dest = jnp.zeros((N_DP * SRC,), jnp.int32).at[target].set(global_slot, mode='drop')
    return (lengths, dest)


def draw_sample_tokens(key, part):
    return plan_tables(key)[0]


def draw_dest_slot(key, part):
    return plan_tables(key)[1]


def draw_loss_mask(key, part):
    row_total = N_DP * SRC
    row_ids = jnp.arange(row_total, dtype=jnp.int32)
    sender = row_ids // SRC
    level = jax.random.randint(jax.random.fold_in(key, 22), (), 15, 86).astype(jnp.int32)
    jitter = jax.random.randint(jax.random.fold_in(key, 23), (N_DP,), 50, 151).astype(jnp.int32)
    ramp = N_DP - 1 + 2 * sender
    threshold = level * ramp * jitter[sender]
    drawn = jax.random.randint(jax.random.fold_in(key, 21), (row_total,), 0, 100 * (3 * N_DP - 3) * 150)
    chosen = (drawn < threshold) | (row_ids % SRC == 0)
    return chosen.astype(jnp.int32)


def with_ends(values, key, low, high):
    dims = values.shape
    index_at = [jax.random.randint(jax.random.fold_in(key, axis), (), 0, dims[axis]) for axis in range(len(dims))]
    values = values.at[tuple(index_at)].set(low)
    longest = dims.index(max(dims))
    index_at[longest] = (index_at[longest] + 1) % dims[longest]
    return values.at[tuple(index_at)].set(high)


def block_levels(own_key, extent, shards, smallest, top_value):
    level, own = 1.0, jax.random.fold_in(own_key, 6)
    for position, parts in shards:
        draws = jnp.exp(jax.random.uniform(jax.random.fold_in(own, position), (parts,), jnp.float32, smallest / len(shards), top_value / len(shards)))
        level = level * jnp.repeat(draws, extent[position] // parts).reshape([-1 if axis == position else 1 for axis in range(len(extent))])
    return level


def bell_draw(own_key, shape, spread, bound, cuts=(), held_as=jnp.bfloat16):
    level = block_levels(own_key, shape, cuts, -0.22, 0.18) if cuts else 1.0
    entries = jax.random.normal(own_key, shape, jnp.float32) * spread * level
    return jnp.minimum(jnp.maximum(entries, -bound), bound).astype(held_as)


def setup_inputs(seed: int = 0) -> dict:
    streams_of = jax.random.split(jax.random.key(seed), 14)
    tokens = bell_draw(streams_of[0], (N_DP * SRC, D), 1.0, 6.0, ((0, 64),))
    positions = with_ends(jax.random.randint(streams_of[1], (3, N_DP * SRC), 0, 2048), jax.random.fold_in(streams_of[1], 1), 0, 2047).astype(jnp.int32)
    loss_mask = draw_loss_mask(jax.random.fold_in(streams_of[13], 71), 0)
    sample_tokens = draw_sample_tokens(jax.random.fold_in(streams_of[13], 71), 0)
    dest_slot = draw_dest_slot(jax.random.fold_in(streams_of[13], 71), 0)
    norm_gain = jnp.clip(1.0 + 0.1 * jax.random.normal(streams_of[5], (D,), jnp.float32), 0.5, 1.5)
    q_weight = bell_draw(streams_of[6], (D, HQ * DH), D ** -0.5, 0.09375, ((1, 4),))
    k_weight = bell_draw(streams_of[7], (D, KV * DH), D ** -0.5, 0.09375, ((1, 4),))
    v_weight = bell_draw(streams_of[8], (D, KV * DH), D ** -0.5, 0.09375, ((1, 4),))
    q_bias = bell_draw(streams_of[9], (HQ * DH,), 0.5, 3.0, ((0, 4),), jnp.float32)
    k_bias = bell_draw(streams_of[10], (KV * DH,), 0.5, 3.0, ((0, 4),), jnp.float32)
    v_bias = bell_draw(streams_of[11], (KV * DH,), 0.5, 3.0, ((0, 4),), jnp.float32)
    o_weight = bell_draw(streams_of[12], (HQ * DH, D), (HQ * DH) ** -0.5, 0.125, ((0, 4),))
    return {"tokens": tokens, "positions": positions, "loss_mask": loss_mask, "sample_tokens": sample_tokens, "dest_slot": dest_slot, "norm_gain": norm_gain, "q_weight": q_weight, "k_weight": k_weight, "v_weight": v_weight, "q_bias": q_bias, "k_bias": k_bias, "v_bias": v_bias, "o_weight": o_weight}


NORM_EPSILON = 1e-06
ROPE_BASE = 1000000.0

def rms_norm(rows_in, gain):
    widened = rows_in.astype(jnp.float32)
    mean_square = lax.optimization_barrier(jnp.mean(widened * widened, axis=-1, keepdims=True))
    return (widened * lax.rsqrt(mean_square + NORM_EPSILON) * gain).astype(jnp.bfloat16)

def rotary_tables(position_ids, head_size):
    half_size = head_size // 2
    pair_index = jnp.arange(half_size, dtype=jnp.int32)
    inv_freq = jnp.exp(pair_index.astype(jnp.float32) * (-2.0 * math.log(ROPE_BASE) / head_size))
    time_limit = head_size // 8
    height_limit = time_limit + 3 * head_size // 16
    chosen = jnp.where(pair_index[None, :] < time_limit, position_ids[0][:, None], jnp.where(pair_index[None, :] < height_limit, position_ids[1][:, None], position_ids[2][:, None]))
    angles = chosen.astype(jnp.float32) * inv_freq[None, :]
    return (jnp.cos(angles), jnp.sin(angles))

def rotate(heads_in, cosine, sine_part):
    half_size = heads_in.shape[-1] // 2
    first_half = heads_in[..., :half_size]
    second_half = heads_in[..., half_size:]
    cosine = cosine[:, None, :]
    sine_part = sine_part[:, None, :]
    return jnp.concatenate([first_half * cosine - second_half * sine_part, second_half * cosine + first_half * sine_part], axis=-1)

def attend_group(queries, key_rows, value_rows, lengths):
    block_count = queries.shape[0]
    row_count = queries.shape[1]
    scores = jnp.einsum('bqagd,bkad->bagqk', queries.astype(jnp.float32), key_rows.astype(jnp.float32)) * (1.0 / math.sqrt(DH))
    places = jnp.arange(row_count, dtype=jnp.int32)
    allowed = (places[:, None] >= places[None, :])[None] & (places[None, None, :] < lengths[:, None, None])
    scores = jnp.where(allowed[:, None, None], scores, -1e+30)
    weights = jax.nn.softmax(scores, axis=-1).astype(jnp.bfloat16)
    context = jnp.einsum('bagqk,bkad->bqagd', weights.astype(jnp.float32), value_rows.astype(jnp.float32))
    live_rows = places[None, :] < lengths[:, None]
    context = jnp.where(live_rows[:, :, None, None, None], context, 0.0).astype(jnp.bfloat16)
    return context.reshape(block_count * row_count, -1)

def attend_buckets(q_rows, k_rows, v_rows, lengths, kv_count, group_size):
    half_bucket = BUCKET // 2
    first_part = attend_group(q_rows[:BUCKET].reshape(1, BUCKET, kv_count, group_size, DH), k_rows[:BUCKET].reshape(1, BUCKET, kv_count, DH), v_rows[:BUCKET].reshape(1, BUCKET, kv_count, DH), lengths[:1])
    second_part = attend_group(q_rows[BUCKET:].reshape(2, half_bucket, kv_count, group_size, DH), k_rows[BUCKET:].reshape(2, half_bucket, kv_count, DH), v_rows[BUCKET:].reshape(2, half_bucket, kv_count, DH), lengths[1:])
    return jnp.concatenate([first_part, second_part], axis=0)

def reference(tokens, positions, loss_mask, sample_tokens, dest_slot, norm_gain, q_weight, k_weight, v_weight, q_bias, k_bias, v_bias, o_weight):
    peer_count = sample_tokens.shape[0]
    slot_count = 2 * BUCKET
    total_slots = peer_count * slot_count
    head_count = q_weight.shape[1] // DH
    kv_count = k_weight.shape[1] // DH
    group_size = head_count // kv_count
    normed = rms_norm(tokens, norm_gain)
    queries = (jnp.dot(normed, q_weight, preferred_element_type=jnp.float32) + q_bias).astype(jnp.bfloat16)
    key_rows = (jnp.dot(normed, k_weight, preferred_element_type=jnp.float32) + k_bias).astype(jnp.bfloat16)
    value_rows = (jnp.dot(normed, v_weight, preferred_element_type=jnp.float32) + v_bias).astype(jnp.bfloat16)
    cosine, sine_part = rotary_tables(positions, DH)
    queries = rotate(queries.astype(jnp.float32).reshape(-1, head_count, DH), cosine, sine_part).astype(jnp.bfloat16)
    key_rows = rotate(key_rows.astype(jnp.float32).reshape(-1, kv_count, DH), cosine, sine_part).astype(jnp.bfloat16)
    q_slots = jnp.zeros((total_slots, head_count * DH), jnp.bfloat16).at[dest_slot].set(queries.reshape(-1, head_count * DH))
    k_slots = jnp.zeros((total_slots, kv_count * DH), jnp.bfloat16).at[dest_slot].set(key_rows.reshape(-1, kv_count * DH))
    v_slots = jnp.zeros((total_slots, kv_count * DH), jnp.bfloat16).at[dest_slot].set(value_rows)

    def attend(inputs):
        q_rows, k_rows, v_rows, lengths = inputs
        return attend_buckets(q_rows, k_rows, v_rows, lengths, kv_count, group_size)
    context = lax.map(attend, (q_slots.reshape(peer_count, slot_count, head_count * DH), k_slots.reshape(peer_count, slot_count, kv_count * DH), v_slots.reshape(peer_count, slot_count, kv_count * DH), sample_tokens))
    context = context.reshape(total_slots, head_count * DH)
    slice_width = head_count * DH // N_SEQ
    head_total = jnp.zeros((total_slots, tokens.shape[1]), jnp.float32)
    for group_index in range(N_SEQ):
        partial_value = jnp.dot(context[:, group_index * slice_width:(group_index + 1) * slice_width], o_weight[group_index * slice_width:(group_index + 1) * slice_width], preferred_element_type=jnp.float32).astype(jnp.bfloat16)
        head_total = head_total + partial_value.astype(jnp.float32)
    mixed = head_total.astype(jnp.bfloat16)
    mask_float = loss_mask.astype(jnp.float32)
    token_count = jnp.sum(mask_float)
    row_scale = tokens.shape[0] / token_count
    token_weight = jnp.zeros((total_slots,), jnp.float32).at[dest_slot].set(mask_float * row_scale)
    return (mixed, token_weight)
```

```python
import functools
import math

import jax
import jax.numpy as jnp
from jax import lax
from jax.experimental import pallas as pl
from jax.experimental.pallas import tpu as pltpu
from jax.sharding import Mesh
from jax.sharding import PartitionSpec as P

DH = 128
BUCKET = 384
DP = ("dp_0", "dp_1", "dp_2")
DP_SEQ = ("dp_0", "dp_1", "dp_2", "seq")
PEERS = 64
SLOTS = 2 * BUCKET
WIDE = 768
HALF = 384
META = 384

NORM_EPSILON = 1e-06
ROPE_BASE = 1000000.0
MESH = pl.DeviceIdType.MESH


def rms_norm(rows_in, gain):
    widened = rows_in.astype(jnp.float32)
    mean_square = jnp.mean(widened * widened, axis=-1, keepdims=True)
    return (widened * lax.rsqrt(mean_square + NORM_EPSILON) * gain).astype(jnp.bfloat16)


def rotary_tables(position_ids, head_size):
    half_size = head_size // 2
    pair_index = jnp.arange(half_size, dtype=jnp.int32)
    inv_freq = jnp.exp(pair_index.astype(jnp.float32) * (-2.0 * math.log(ROPE_BASE) / head_size))
    time_limit = head_size // 8
    height_limit = time_limit + 3 * head_size // 16
    chosen = jnp.where(
        pair_index[None, :] < time_limit,
        position_ids[0][:, None],
        jnp.where(
            pair_index[None, :] < height_limit, position_ids[1][:, None], position_ids[2][:, None]
        ),
    )
    angles = chosen.astype(jnp.float32) * inv_freq[None, :]
    return (jnp.cos(angles), jnp.sin(angles))


def rotate(heads_in, cosine, sine_part):
    half_size = heads_in.shape[-1] // 2
    first_half = heads_in[..., :half_size]
    second_half = heads_in[..., half_size:]
    cosine = cosine[:, None, :]
    sine_part = sine_part[:, None, :]
    return jnp.concatenate(
        [
            first_half * cosine - second_half * sine_part,
            second_half * cosine + first_half * sine_part,
        ],
        axis=-1,
    )


def attend_group(queries, key_rows, value_rows, lengths):
    block_count = queries.shape[0]
    row_count = queries.shape[1]
    scores = jnp.einsum(
        "bqagd,bkad->bagqk", queries, key_rows, preferred_element_type=jnp.float32
    ) * (1.0 / math.sqrt(DH))
    places = jnp.arange(row_count, dtype=jnp.int32)
    allowed = (places[:, None] >= places[None, :])[None] & (
        places[None, None, :] < lengths[:, None, None]
    )
    scores = jnp.where(allowed[:, None, None], scores, -1e30)
    weights = jax.nn.softmax(scores, axis=-1).astype(jnp.bfloat16)
    context = jnp.einsum(
        "bagqk,bkad->bqagd", weights, value_rows, preferred_element_type=jnp.float32
    )
    live_rows = places[None, :] < lengths[:, None]
    context = jnp.where(live_rows[:, :, None, None, None], context, 0.0).astype(jnp.bfloat16)
    return context.reshape(block_count * row_count, -1)


def attend_buckets(q_rows, k_rows, v_rows, lengths, kv_count, group_size):
    half_bucket = BUCKET // 2
    first_part = attend_group(
        q_rows[:BUCKET].reshape(1, BUCKET, kv_count, group_size, DH),
        k_rows[:BUCKET].reshape(1, BUCKET, kv_count, DH),
        v_rows[:BUCKET].reshape(1, BUCKET, kv_count, DH),
        lengths[:1],
    )
    second_part = attend_group(
        q_rows[BUCKET:].reshape(2, half_bucket, kv_count, group_size, DH),
        k_rows[BUCKET:].reshape(2, half_bucket, kv_count, DH),
        v_rows[BUCKET:].reshape(2, half_bucket, kv_count, DH),
        lengths[1:],
    )
    return jnp.concatenate([first_part, second_part], axis=0)


def peer_coords(index):
    return {"dp_0": index // 8, "dp_1": lax.rem(index // 2, 4), "dp_2": lax.rem(index, 2)}


def exchange_kernel(main_in, tail_in, meta_in, main_out, tail_out, meta_out, send_sems, recv_sems, own_sems):
    me = (lax.axis_index("dp_0") * 4 + lax.axis_index("dp_1")) * 2 + lax.axis_index("dp_2")
    pairs = ((meta_in, meta_out), (main_in, main_out), (tail_in, tail_out))
    barrier = pltpu.get_barrier_semaphore()

    @pl.loop(1, PEERS)
    def _(step):
        peer = lax.rem(me + step, PEERS)
        pl.semaphore_signal(barrier, inc=1, device_id=peer_coords(peer), device_id_type=MESH)

    own = [
        pltpu.make_async_copy(src.at[me], dst.at[me], own_sems.at[i])
        for i, (src, dst) in enumerate(pairs)
    ]
    for copy in own:
        copy.start()
    pl.semaphore_wait(barrier, PEERS - 1)

    @pl.loop(1, PEERS)
    def _(step):
        peer = lax.rem(me + step, PEERS)
        for i, (src, dst) in enumerate(pairs):
            pltpu.make_async_remote_copy(
                src_ref=src.at[peer],
                dst_ref=dst.at[me],
                send_sem=send_sems.at[i],
                recv_sem=recv_sems.at[i],
                device_id=peer_coords(peer),
                device_id_type=MESH,
            ).start()

    for copy in own:
        copy.wait()
    for i, (src, dst) in enumerate(pairs):
        whole = dst.at[pl.ds(0, PEERS - 1)]
        pltpu.make_async_copy(whole, whole, recv_sems.at[i]).wait()
        whole = src.at[pl.ds(0, PEERS - 1)]
        pltpu.make_async_copy(whole, whole, send_sems.at[i]).wait()


def exchange(main, tail, meta):
    shapes = [jax.ShapeDtypeStruct(a.shape, a.dtype) for a in (main, tail, meta)]
    return pl.pallas_call(
        exchange_kernel,
        out_shape=shapes,
        in_specs=[pl.BlockSpec(memory_space=pl.ANY)] * 3,
        out_specs=[pl.BlockSpec(memory_space=pl.ANY)] * 3,
        scratch_shapes=[
            pltpu.SemaphoreType.DMA((3,)),
            pltpu.SemaphoreType.DMA((3,)),
            pltpu.SemaphoreType.DMA((3,)),
        ],
        compiler_params=pltpu.CompilerParams(collective_id=0, has_side_effects=True),
    )(main, tail, meta)


def per_device(
    tokens,
    positions,
    loss_mask,
    sample_tokens,
    dest_slot,
    norm_gain,
    q_weight,
    k_weight,
    v_weight,
    q_bias,
    k_bias,
    v_bias,
    o_weight,
):
    own_index = lax.axis_index(DP)
    seq_count = lax.axis_size("seq")
    seq_index = lax.axis_index("seq")
    source_rows = tokens.shape[0]
    head_count = q_weight.shape[1] // DH
    kv_count = k_weight.shape[1] // DH
    group_size = head_count // kv_count
    bf16, f32 = jnp.bfloat16, jnp.float32

    peer = dest_slot // SLOTS
    value = (dest_slot % SLOTS) * 2 + loss_mask + 1
    rows = jnp.arange(source_rows, dtype=jnp.int32)
    same = (peer[:, None] == peer[None, :]) & (rows[:, None] > rows[None, :])
    rank = jnp.sum(same.astype(jnp.int32), axis=1)

    out_row = jnp.arange(PEERS * 8, dtype=jnp.int32)
    out_peer, out_lane = out_row // 8, out_row % 8
    hit = out_peer[:, None] == peer[None, :]
    pick_main = (hit & (out_lane[:, None] == rank[None, :])).astype(bf16)
    pick_tail = (hit & ((out_lane % 4)[:, None] + 8 == rank[None, :])).astype(bf16)
    meta_rank = jnp.arange(256, dtype=jnp.int32)
    meta_rank = jnp.where(meta_rank < 128, meta_rank % 8, 8 + meta_rank % 4)
    to_peer = (jnp.arange(PEERS, dtype=jnp.int32)[:, None] == peer[None, :]).astype(f32)
    spread = jnp.where(rank[:, None] == meta_rank[None, :], value[:, None], 0).astype(f32)
    meta = jnp.dot(to_peer, spread, precision=lax.Precision.HIGHEST).astype(jnp.int32)
    mask_sum = jnp.broadcast_to(jnp.sum(loss_mask), (PEERS, 128))
    meta = jnp.concatenate([meta, mask_sum], axis=1).reshape(PEERS, 1, META)

    normed = rms_norm(tokens, norm_gain)
    weight = jnp.concatenate([q_weight, k_weight, v_weight], axis=1)
    bias = jnp.concatenate([q_bias, k_bias, v_bias])
    qkv = (jnp.dot(normed, weight, preferred_element_type=f32) + bias).astype(bf16)
    cosine, sine = rotary_tables(positions, DH)
    turned = rotate(qkv[:, :640].astype(f32).reshape(source_rows, 5, DH), cosine, sine)
    qkv = jnp.concatenate([turned.astype(bf16).reshape(source_rows, 640), qkv[:, 640:]], axis=1)

    main = jnp.dot(pick_main, qkv, preferred_element_type=f32).astype(bf16)
    tail = jnp.dot(pick_tail, qkv, preferred_element_type=f32).astype(bf16)
    tail = jnp.where((out_lane < 4)[:, None], tail[:, :HALF], tail[:, HALF:])
    main, tail, meta = exchange(
        main.reshape(PEERS, 8, WIDE), tail.reshape(PEERS, 8, HALF), meta
    )
    main, tail = main.reshape(PEERS * 8, WIDE), tail.reshape(PEERS * 8, HALF)
    main_value = meta[:, 0, :8].reshape(-1)
    tail_value = meta[:, 0, 128:136].reshape(-1)
    loss_total = jnp.sum(meta[:, 0, 256]).astype(f32)

    slot = jnp.arange(SLOTS, dtype=jnp.int32)[:, None]
    put_main = slot * 2 + 1 == main_value - (main_value - 1) % 2
    put_main = put_main & (main_value > 0)
    put_tail = (slot * 2 + 1 == tail_value - (tail_value - 1) % 2) & (tail_value > 0)
    put_low = put_tail & (out_lane < 4)
    put_high = put_tail & (out_lane >= 4)
    placed = jnp.dot(put_main.astype(bf16), main, preferred_element_type=f32) + jnp.concatenate(
        [
            jnp.dot(put_low.astype(bf16), tail, preferred_element_type=f32),
            jnp.dot(put_high.astype(bf16), tail, preferred_element_type=f32),
        ],
        axis=1,
    )
    placed = placed.astype(bf16)
    flags = jnp.sum(jnp.where(put_main, (main_value - 1) % 2, 0), axis=1) + jnp.sum(
        jnp.where(put_low, (tail_value - 1) % 2, 0), axis=1
    )

    lengths = sample_tokens[own_index]
    context = attend_buckets(
        placed[:, :512], placed[:, 512:640], placed[:, 640:], lengths, kv_count, group_size
    )
    part_rows = SLOTS // seq_count
    mixed = lax.psum_scatter(
        jnp.dot(context, o_weight, preferred_element_type=jnp.float32).astype(jnp.bfloat16),
        "seq",
        scatter_dimension=0,
        tiled=True,
    )
    row_scale = PEERS * source_rows / loss_total
    own_mask = lax.dynamic_slice_in_dim(flags, seq_index * part_rows, part_rows, 0).astype(f32)
    return (mixed, own_mask * row_scale)


def solution(mesh):
    finer = Mesh(mesh.devices.reshape(8, 4, 2, mesh.shape["seq"]), ("dp_0", "dp_1", "dp_2", "seq"))
    placed = (
        P(DP, None),
        P(None, DP),
        P(DP),
        P(),
        P(DP),
        P(),
        P(None, "seq"),
        P(None, "seq"),
        P(None, "seq"),
        P("seq"),
        P("seq"),
        P("seq"),
        P("seq", None),
    )
    return jax.shard_map(
        per_device,
        mesh=finer,
        in_specs=placed,
        out_specs=(P(DP_SEQ, None), P(DP_SEQ)),
        check_vma=False,
    )
```
